256 devices in a mesh: row: 32 (over z, y), col: 8 (over x, core).
Axes of the slice: x: 4, y: 4, z: 8, core: 2. Of those that a mesh axis runs over, the one named last changes fastest.
Arguments:
- features: bfloat16 [32768, 512], P(('col', 'row')), may hold values from -6 to 6
- weight: bfloat16 [512, 512], replicated, may hold values from -0.25 to 0.25
- cotangent: bfloat16 [32768, 512], P(('row', 'col')), may hold values from -6 to 6
- blocks: bfloat16 [32, 8, 128, 128, 128], P('row', 'col'), may hold values from -6 to 6
- block_scales: float32 [32, 8, 128], P('row', 'col'), as said below
- block_rows: int32 [32, 8, 128], P('row', 'col'), may hold values from 0 to 7, as said below
- block_cols: int32 [32, 8, 128], P('row', 'col'), may hold values from 0 to 31, as said below
- block_counts: int32 [32, 8], P('row', 'col'), may hold values from 1 to 128, as said below
Outputs:
- activated: bfloat16 [32768, 512], P(('row', 'col'))
- input_grad: bfloat16 [32768, 512], P(('col', 'row'))
- weight_grad: float32 [512, 512], P(('row', 'col'))
The draws below stay inside these ranges and needn't reach their ends.
Inputs may be any that keep to these rules, and one draw needn't show every extreme that they name: `block_rows`: within one grid cell the 128 slots name distinct block positions. `block_cols`: within one grid cell the 128 slots name distinct block positions. `block_counts`: in every draw some grid cell has all 128 slots live. `block_scales`: Positive.
All inputs are finite; a program needn't handle non-finite values.
Results may differ from the reference program's by a relative error of at most 0.0063.
Values may be sent and summed in bfloat16 or wider, within the bound.
No kernel may reach another device: no remote copies, remote signals or barrier semaphores. Data moves between devices by JAX's collectives and lax.ppermute only.
A program may use at most 64 MiB of HBM per device.

```python
import math
import jax
import jax.numpy as jnp
from jax import lax

FEAT = 512
BLOCK = 128
NODE_DEV = 128
NODES = 32768
BROWS = 8
BCOLS = 32
SLOTS = 128
N_ROW = 32
N_COL = 8


def block_layout(key):
    device_keys = jax.random.split(jax.random.fold_in(key, 7), N_ROW * N_COL)

    def one_device(device_key):
        return jax.random.permutation(device_key, BROWS * BCOLS)[:SLOTS]
    places = jax.vmap(one_device)(device_keys).astype(jnp.int32)
    return places.reshape(N_ROW, N_COL, SLOTS)


def draw_block_rows(key, part):
    return (block_layout(key) // BCOLS).astype(jnp.int32)


def draw_block_cols(key, part):
    return (block_layout(key) % BCOLS).astype(jnp.int32)


def draw_block_counts(key, part):
    first_draw = jax.random.randint(jax.random.fold_in(key, 1), (N_ROW * N_COL,), 1, SLOTS + 1)
    second_draw = jax.random.randint(jax.random.fold_in(key, 2), (N_ROW * N_COL,), 1, SLOTS + 1)
    counts = jnp.minimum(first_draw, second_draw)
    busiest = jax.random.randint(jax.random.fold_in(key, 3), (), 0, N_ROW * N_COL)
    counts = jnp.where(jnp.arange(N_ROW * N_COL) == busiest, SLOTS, counts)
    return counts.reshape(N_ROW, N_COL).astype(jnp.int32)


def draw_block_scales(key, part):
    level = (SLOTS * BLOCK * BLOCK / NODE_DEV) ** (-0.5)
    uniform_part = jax.random.uniform(jax.random.fold_in(key, 11), (N_ROW, N_COL, SLOTS), jnp.float32)
    return (level * jnp.exp(uniform_part * math.log(4.0))).astype(jnp.float32)


def block_scale(rng, extent, shards, least, top_value):
    loudness, own = 1.0, jax.random.fold_in(rng, 6)
    for dim, blocks in shards:
        steps = jnp.exp(jax.random.uniform(jax.random.fold_in(own, dim), (blocks,), jnp.float32, least / len(shards), top_value / len(shards)))
        loudness = loudness * jnp.repeat(steps, extent[dim] // blocks).reshape([-1 if axis == dim else 1 for axis in range(len(extent))])
    return loudness


def noise(key, dims, width, reach, cuts=(), kind=jnp.bfloat16):
    array = width * jax.random.normal(key, dims, jnp.float32)
    if cuts:
        array = array * block_scale(key, dims, cuts, -0.22, 0.18)
    return jnp.clip(array, -reach, reach).astype(kind)


def setup_inputs(seed: int = 0) -> dict:
    splits = jax.random.split(jax.random.key(seed), 9)
    return {
        "features": noise(splits[0], (NODES, FEAT), 1.0, 6.0, ((0, 256),)),
        "weight": noise(splits[1], (FEAT, FEAT), FEAT ** -0.5, 0.25),
        "cotangent": noise(splits[2], (NODES, FEAT), 1.0, 6.0, ((0, 256),)),
        "blocks": noise(splits[3], (N_ROW, N_COL, SLOTS, BLOCK, BLOCK), 1.0, 6.0, ((0, 32), (1, 8))),
        "block_scales": draw_block_scales(jax.random.fold_in(splits[8], 71), 0),
        "block_rows": draw_block_rows(jax.random.fold_in(splits[8], 71), 0),
        "block_cols": draw_block_cols(jax.random.fold_in(splits[8], 71), 0),
        "block_counts": draw_block_counts(jax.random.fold_in(splits[8], 71), 0),
    }


def silu_slope(values):
    sigmoid_part = jax.nn.sigmoid(values)
    return sigmoid_part * (1.0 + values * (1.0 - sigmoid_part))

def reference(features, weight, cotangent, blocks, block_scales, block_rows, block_cols, block_counts):
    tile_rows = NODE_DEV * N_COL
    tile_cols = NODE_DEV * N_ROW
    projected = jnp.dot(features, weight, preferred_element_type=jnp.float32).astype(jnp.bfloat16)
    slot_index = jnp.arange(SLOTS, dtype=jnp.int32)

    def device_parts(device):
        grid_row = device // N_COL
        grid_col = device % N_COL
        adj_tiles = blocks[grid_row, grid_col].astype(jnp.float32)
        live_mask = (slot_index < block_counts[grid_row, grid_col]).astype(jnp.float32)
        factor = block_scales[grid_row, grid_col] * live_mask
        return (grid_row, grid_col, adj_tiles, factor)

    def forward_step(device, summed):
        grid_row, grid_col, adj_tiles, factor = device_parts(device)
        col_start = (grid_col * tile_cols).astype(jnp.int32)
        feature_rows = lax.dynamic_slice_in_dim(projected, col_start, tile_cols, 0).astype(jnp.float32)
        feature_rows = feature_rows.reshape(BCOLS, BLOCK, FEAT)
        chosen = jnp.take(feature_rows, block_cols[grid_row, grid_col], axis=0)
        products = jnp.einsum('gij,gjf->gif', adj_tiles, chosen) * factor[:, None, None]
        tile_sum = jnp.zeros((BROWS, BLOCK, FEAT), jnp.float32).at[block_rows[grid_row, grid_col]].add(products)
        row_start = (grid_row * tile_rows).astype(jnp.int32)
        current = lax.dynamic_slice_in_dim(summed, row_start, tile_rows, 0)
        return lax.dynamic_update_slice_in_dim(summed, current + tile_sum.reshape(tile_rows, FEAT), row_start, 0)
    aggregated = lax.fori_loop(0, N_ROW * N_COL, forward_step, jnp.zeros((NODES, FEAT), jnp.float32))
    activated = jax.nn.silu(aggregated).astype(jnp.bfloat16)
    pre_grad = (cotangent.astype(jnp.float32) * silu_slope(aggregated)).astype(jnp.bfloat16)

    def backward_step(device, summed):
        grid_row, grid_col, adj_tiles, factor = device_parts(device)
        row_start = (grid_row * tile_rows).astype(jnp.int32)
        grad_rows = lax.dynamic_slice_in_dim(pre_grad, row_start, tile_rows, 0).astype(jnp.float32)
        grad_rows = grad_rows.reshape(BROWS, BLOCK, FEAT)
        chosen = jnp.take(grad_rows, block_rows[grid_row, grid_col], axis=0)
        products = jnp.einsum('gji,gjf->gif', adj_tiles, chosen) * factor[:, None, None]
        tile_sum = jnp.zeros((BCOLS, BLOCK, FEAT), jnp.float32).at[block_cols[grid_row, grid_col]].add(products)
        col_start = (grid_col * tile_cols).astype(jnp.int32)
        current = lax.dynamic_slice_in_dim(summed, col_start, tile_cols, 0)
        return lax.dynamic_update_slice_in_dim(summed, current + tile_sum.reshape(tile_cols, FEAT), col_start, 0)
    proj_sum = lax.fori_loop(0, N_ROW * N_COL, backward_step, jnp.zeros((NODES, FEAT), jnp.float32))
    proj_grad = proj_sum.astype(jnp.bfloat16)
    input_grad = lax.dot_general(proj_grad, weight, (((1,), (1,)), ((), ())), preferred_element_type=jnp.float32).astype(jnp.bfloat16)
    weight_grad = lax.dot_general(features, proj_grad, (((0,), (0,)), ((), ())), preferred_element_type=jnp.float32)
    weight_grad = weight_grad * (1.0 / math.sqrt(NODES))
    return (activated, input_grad, weight_grad)
```

```python
import math

import jax
import jax.numpy as jnp
import numpy as np
from jax import lax
from jax.experimental import pallas as pl
from jax.experimental.pallas import tpu as pltpu
from jax.sharding import Mesh
from jax.sharding import PartitionSpec as P

BF = jnp.bfloat16
F32 = jnp.float32
NZ, NY, NX, NC = 8, 4, 4, 2
ROW = ("z", "y")
COL = ("x", "c")
BLK = 128
BROWS = NX * NC
BCOLS = NZ * NY
FEAT = 512


def build_kernel(cnt, rows, cols, scl, blk, dense, dense_t):
    dense[...] = jnp.zeros_like(dense)
    dense_t[...] = jnp.zeros_like(dense_t)

    def one(s, carry):
        r, c = rows[s], cols[s]
        tile = blk[s].astype(F32) * scl[s]
        ct = (c % NY) * NZ + c // NY
        r0 = pl.multiple_of(r * BLK, BLK)
        c0 = pl.multiple_of(c * BLK, BLK)
        t0 = pl.multiple_of(ct * BLK, BLK)
        dense[pl.ds(r0, BLK), pl.ds(c0, BLK)] = tile.astype(BF)
        dense_t[pl.ds(t0, BLK), pl.ds(r0, BLK)] = tile.T.astype(BF)
        return carry

    lax.fori_loop(0, cnt[0], one, 0)


def build(cnt, rows, cols, scl, blk):
    smem = pl.BlockSpec(memory_space=pltpu.SMEM)
    vmem = pl.BlockSpec(memory_space=pltpu.VMEM)
    return pl.pallas_call(
        build_kernel,
        out_shape=(
            jax.ShapeDtypeStruct((BROWS * BLK, BCOLS * BLK), BF),
            jax.ShapeDtypeStruct((BCOLS * BLK, BROWS * BLK), BF),
        ),
        in_specs=[smem, smem, smem, smem, vmem],
        out_specs=(vmem, vmem),
        compiler_params=pltpu.CompilerParams(vmem_limit_bytes=40 << 20),
        cost_estimate=pl.CostEstimate(flops=1 << 22, bytes_accessed=20 << 20, transcendentals=0),
    )(cnt, rows, cols, scl, blk)


def shards(features, weight, cotangent, blocks, block_scales, block_rows, block_cols, block_counts):
    cnt = block_counts.reshape(1)
    dense, dense_t = build(
        cnt, block_rows.reshape(-1), block_cols.reshape(-1), block_scales.reshape(-1), blocks[0, 0]
    )
    feat_y = lax.all_gather(features, "y", axis=0, tiled=True)
    feat = lax.all_gather(feat_y, "z", axis=0, tiled=True)
    part = jnp.dot(dense, feat, preferred_element_type=F32).astype(BF)
    part = lax.all_to_all(part.reshape(BROWS, BLK, FEAT), COL, 0, 0)
    hid = jnp.sum(part.astype(F32), axis=0).astype(BF)
    agg = jnp.dot(hid, weight, preferred_element_type=F32)
    sig = jax.nn.sigmoid(agg)
    activated = (agg * sig).astype(BF)
    pre = (cotangent.astype(F32) * (sig * (1.0 + agg * (1.0 - sig)))).astype(BF)
    wpart = lax.dot_general(hid, pre, (((0,), (0,)), ((), ())), preferred_element_type=F32).astype(BF)
    grad = lax.dot_general(pre, weight, (((1,), (1,)), ((), ())), preferred_element_type=F32).astype(BF)
    grad = lax.all_gather(grad, COL, axis=0, tiled=True)
    wall = lax.all_to_all(wpart.reshape(NZ * NY * NX * NC, 2, FEAT), ROW + COL, 0, 0)
    nodes = BLK * NZ * NY * NX * NC
    weight_grad = jnp.sum(wall.astype(F32), axis=0) * (1.0 / math.sqrt(nodes))
    back = jnp.dot(dense_t, grad, preferred_element_type=F32).astype(BF)
    back = lax.all_to_all(back.reshape(NY, NZ * BLK, FEAT), "y", 0, 0)
    back = jnp.sum(back.astype(F32), axis=0).astype(BF)
    back = lax.all_to_all(back.reshape(NZ, BLK, FEAT), "z", 0, 0)
    input_grad = jnp.sum(back.astype(F32), axis=0).astype(BF)
    return (activated, input_grad, weight_grad)


def solution(mesh):
    mesh4 = Mesh(np.asarray(mesh.devices).reshape(NZ, NY, NX, NC), ("z", "y", "x", "c"))
    return jax.shard_map(
        shards,
        mesh=mesh4,
        in_specs=(
            P(COL + ROW, None),
            P(),
            P(ROW + COL, None),
            P(ROW, COL, None, None, None),
            P(ROW, COL, None),
            P(ROW, COL, None),
            P(ROW, COL, None),
            P(ROW, COL),
        ),
        out_specs=(P(ROW + COL, None), P(COL + ROW, None), P(ROW + COL, None)),
        check_vma=False,
    )
```

```python
import math

import jax
import jax.numpy as jnp
import numpy as np
from jax import lax
from jax.experimental import pallas as pl
from jax.experimental.pallas import tpu as pltpu
from jax.sharding import Mesh
from jax.sharding import PartitionSpec as P

BF = jnp.bfloat16
F32 = jnp.float32
NZ, NY, NX, NC = 8, 4, 4, 2
ROW = ("z", "y")
COL = ("x", "c")
SIZES = {"z": NZ, "y": NY, "x": NX, "c": NC}
BLK = 128
FEAT = 512
YB = NY * BLK
RB = NX * NC * BLK


def hop(value, axis, step):
    n = SIZES[axis]
    return lax.ppermute(value, axis, [(i, (i + step) % n) for i in range(n)])


def build_kernel(cnt, rows, cols, pos, scl, blk, dense, dense_t):
    dense[...] = jnp.zeros_like(dense)
    dense_t[...] = jnp.zeros_like(dense_t)
    z, y, x, c = pos[0], pos[1], pos[2], pos[3]

    def one(s, carry):
        rb, cb = rows[s], cols[s]
        dx = (rb // NC - x + NX) % NX
        dc = (rb % NC + c) % NC
        dz = (cb // NY - z + NZ) % NZ
        yc = cb % NY
        dy = (yc - y + NY) % NY
        tile = blk[s].astype(F32) * scl[s]
        r0 = pl.multiple_of((dc * NX + dx) * BLK, BLK)
        c0 = pl.multiple_of(yc * BLK, BLK)
        t0 = pl.multiple_of(dy * BLK, BLK)
        dense[dz, pl.ds(r0, BLK), pl.ds(c0, BLK)] = tile.astype(BF)
        dense_t[dz, pl.ds(t0, BLK), pl.ds(r0, BLK)] = tile.T.astype(BF)
        return carry

    lax.fori_loop(0, cnt[0], one, 0)


def build(cnt, rows, cols, pos, scl, blk):
    smem = pl.BlockSpec(memory_space=pltpu.SMEM)
    vmem = pl.BlockSpec(memory_space=pltpu.VMEM)
    return pl.pallas_call(
        build_kernel,
        out_shape=(
            jax.ShapeDtypeStruct((NZ, RB, YB), BF),
            jax.ShapeDtypeStruct((NZ, YB, RB), BF),
        ),
        in_specs=[smem, smem, smem, smem, smem, vmem],
        out_specs=(vmem, vmem),
        compiler_params=pltpu.CompilerParams(vmem_limit_bytes=40 << 20),
        cost_estimate=pl.CostEstimate(flops=1 << 22, bytes_accessed=20 << 20, transcendentals=0),
    )(cnt, rows, cols, pos, scl, blk)


def mm(a, b):
    return jnp.dot(a, b, preferred_element_type=F32)


def shards(features, weight, cotangent, blocks, block_scales, block_rows, block_cols, block_counts):
    cnt = block_counts.reshape(1)
    pos = jnp.stack([lax.axis_index(a) for a in ("z", "y", "x", "c")]).astype(jnp.int32)
    f0 = lax.all_gather(features, "y", axis=0, tiled=True)
    up1, dn1 = hop(f0, "z", 1), hop(f0, "z", -1)
    dense, dense_t = build(
        cnt, block_rows.reshape(-1), block_cols.reshape(-1), pos, block_scales.reshape(-1), blocks[0, 0]
    )
    acc = mm(dense[0], f0)
    up2, dn2 = hop(up1, "z", 1), hop(dn1, "z", -1)
    acc = acc + mm(dense[7], up1) + mm(dense[1], dn1)
    up3, dn3 = hop(up2, "z", 1), hop(dn2, "z", -1)
    acc = acc + mm(dense[6], up2) + mm(dense[2], dn2)
    half = YB // 2
    up4, dn4 = hop(up3[:half], "z", 1), hop(dn3[half:], "z", -1)
    acc = acc + mm(dense[5], up3) + mm(dense[3], dn3)
    acc = acc + mm(dense[4, :, :half], up4) + mm(dense[4, :, half:], dn4)
    mine = acc[: RB // 2] + hop(acc[RB // 2 :].astype(BF), "c", 1).astype(F32)
    sent = mine.astype(BF)
    parts = [hop(sent[d * BLK : (d + 1) * BLK], "x", d) for d in range(1, NX)]
    hid = mine[:BLK]
    for p in parts:
        hid = hid + p.astype(F32)
    hid = hid.astype(BF)
    agg = mm(hid, weight)
    sig = jax.nn.sigmoid(agg)
    activated = (agg * sig).astype(BF)
    pre = (cotangent.astype(F32) * (sig * (1.0 + agg * (1.0 - sig)))).astype(BF)
    grad = lax.dot_general(pre, weight, (((1,), (1,)), ((), ())), preferred_element_type=F32).astype(BF)
    own = jnp.concatenate([grad] + [hop(grad, "x", -d) for d in range(1, NX)], axis=0)
    other = hop(own, "c", 1)
    wpart = lax.dot_general(hid, pre, (((0,), (0,)), ((), ())), preferred_element_type=F32).astype(BF)
    wall = lax.all_to_all(wpart.reshape(NZ * NY * NX * NC, 2, FEAT), ROW + COL, 0, 0)
    nodes = BLK * NZ * NY * NX * NC
    weight_grad = jnp.sum(wall.astype(F32), axis=0) * (1.0 / math.sqrt(nodes))

    def piece(dz, lo=0, hi=YB):
        return mm(dense_t[dz, lo:hi, : RB // 2], own) + mm(dense_t[dz, lo:hi, RB // 2 :], other)

    up = hop(piece(4, 0, half).astype(BF), "z", 1)
    dn = hop(piece(4, half, YB).astype(BF), "z", -1)
    zero = jnp.zeros((half, FEAT), BF)
    up, dn = jnp.concatenate([up, zero]), jnp.concatenate([zero, dn])
    for d in (3, 2, 1):
        up = hop((piece(d) + up.astype(F32)).astype(BF), "z", 1)
        dn = hop((piece(NZ - d) + dn.astype(F32)).astype(BF), "z", -1)
    total = piece(0) + up.astype(F32) + dn.astype(F32)
    sent = total.astype(BF)
    parts = [hop(sent[d * BLK : (d + 1) * BLK], "y", d) for d in range(1, NY)]
    input_grad = total[:BLK]
    for p in parts:
        input_grad = input_grad + p.astype(F32)
    return (activated, input_grad.astype(BF), weight_grad)


def solution(mesh):
    mesh4 = Mesh(np.asarray(mesh.devices).reshape(NZ, NY, NX, NC), ("z", "y", "x", "c"))
    return jax.shard_map(
        shards,
        mesh=mesh4,
        in_specs=(
            P(COL + ROW, None),
            P(),
            P(ROW + COL, None),
            P(ROW, COL, None, None, None),
            P(ROW, COL, None),
            P(ROW, COL, None),
            P(ROW, COL, None),
            P(ROW, COL),
        ),
        out_specs=(P(ROW + COL, None), P(COL + ROW, None), P(ROW + COL, None)),
        check_vma=False,
    )
```

```python
import functools
import math

import jax
import jax.numpy as jnp
import numpy as np
from jax import lax
from jax.experimental import pallas as pl
from jax.experimental.pallas import tpu as pltpu
from jax.sharding import Mesh
from jax.sharding import PartitionSpec as P

BF = jnp.bfloat16
F32 = jnp.float32
NZ, NY, NX, NC = 8, 4, 4, 2
ROW = ("z", "y")
COL = ("x", "c")
SIZES = {"z": NZ, "y": NY, "x": NX, "c": NC}
BLK = 128
FEAT = 512
YB = NY * BLK
RB = NX * NC * BLK
GROUP = 4
MROWS = 256


def hop(value, axis, step):
    n = SIZES[axis]
    return lax.ppermute(value, axis, [(i, (i + step) % n) for i in range(n)])


def place(pos, rb, cb):
    dx = (rb // NC - pos[2] + NX) % NX
    dc = (rb % NC + pos[3]) % NC
    dz = (cb // NY - pos[0] + NZ) % NZ
    dy = (cb % NY - pos[1] + NY) % NY
    return pl.multiple_of((dc * NX + dx) * BLK, BLK), dz, pl.multiple_of(dy * BLK, BLK)


def build_kernel(cnt, rows, cols, pos, scl, blk, dense, transpose=False):
    dense[...] = jnp.zeros_like(dense)

    def group(g, carry):
        for j in range(GROUP):
            s = g * GROUP + j
            r0, dz, c0 = place(pos, rows[s], cols[s])
            factor = jnp.where(s < cnt[0], scl[s], 0.0)
            tile = (blk[s].astype(F32) * factor).astype(BF)
            if transpose:
                dense[dz, pl.ds(c0, BLK), pl.ds(r0, BLK)] = tile.T
            else:
                dense[dz, pl.ds(r0, BLK), pl.ds(c0, BLK)] = tile
        return carry

    lax.fori_loop(0, (cnt[0] + GROUP - 1) // GROUP, group, 0)


SMEM = pl.BlockSpec(memory_space=pltpu.SMEM)
VMEM = pl.BlockSpec(memory_space=pltpu.VMEM)


def call(kernel, outs, n_smem, flops, *args, aliases=None, scratch=()):
    n_vmem = len(args) - n_smem
    return pl.pallas_call(
        kernel,
        out_shape=outs,
        in_specs=[SMEM] * n_smem + [VMEM] * n_vmem,
        out_specs=jax.tree.map(lambda _: VMEM, outs),
        scratch_shapes=list(scratch),
        input_output_aliases=aliases or {},
        compiler_params=pltpu.CompilerParams(vmem_limit_bytes=(12 if scratch else 4) << 20),
        cost_estimate=pl.CostEstimate(flops=flops, bytes_accessed=1 << 20, transcendentals=0),
    )(*args)


def build_dense(*args):
    return call(build_kernel, jax.ShapeDtypeStruct((NZ, RB, YB), BF), 5, 1 << 32, *args)


def build_t_kernel(cnt, rows, cols, pos, scl, blk, *refs):
    dense = refs[-1]
    build_kernel(cnt, rows, cols, pos, scl, blk, dense, transpose=True)
    for dz in range(NZ):
        refs[dz][...] = dense[dz]


def build_dense_t(*args):
    outs = tuple(jax.ShapeDtypeStruct((YB, RB), BF) for _ in range(NZ))
    return call(build_t_kernel, outs, 5, 1 << 33, *args, scratch=[pltpu.VMEM((NZ, YB, RB), BF)])


def mm(a, b):
    return jnp.dot(a, b, preferred_element_type=F32)


def after(value, *deps):
    return lax.optimization_barrier((value,) + deps)[0]


def out(rows, dtype):
    return jax.ShapeDtypeStruct((rows, FEAT), dtype)


def forward(dense, spans, pieces, acc, last):
    n = len(spans)
    has_acc = acc is not None

    def kernel(*refs):
        tile, f = refs[0], refs[1 : 1 + n]
        outs = refs[1 + n + has_acc :]
        rhs = jnp.concatenate([r[...] for r in f], axis=0)

        def rows(m, carry):
            at = pl.ds(pl.multiple_of(m * MROWS, MROWS), MROWS)
            lhs = jnp.concatenate([tile[dz, at, lo:hi] for dz, lo, hi in spans], axis=1)
            value = mm(lhs, rhs)
            if has_acc:
                value = value + refs[1 + n][at, :]
            if not last:
                outs[0][at, :] = value
                return carry
            half = RB // 2 // MROWS

            @pl.when(m < half)
            def _():
                outs[0][at, :] = value

            @pl.when(m >= half)
            def _():
                outs[1][pl.ds(pl.multiple_of((m - half) * MROWS, MROWS), MROWS), :] = value.astype(BF)

            return carry

        lax.fori_loop(0, RB // MROWS, rows, 0)

    outs = (out(RB // 2, F32), out(RB // 2, BF)) if last else out(RB, F32)
    args = (dense, *pieces) + ((acc,) if has_acc else ())
    flops = 2 * RB * FEAT * sum(hi - lo for _, lo, hi in spans)
    return call(kernel, outs, 0, flops, *args, aliases={1 + n: 0} if has_acc and not last else None)


def backward(dense_t, grads, dz, lo, hi, adds, dtype):
    n = len(grads)

    def kernel(*refs):
        tile, g, got, result = refs[0], refs[1 : 1 + n], refs[1 + n : -1], refs[-1]
        rhs = jnp.concatenate([r[...] for r in g], axis=0)
        for m in range((hi - lo) // BLK):
            value = mm(tile[lo + m * BLK : lo + (m + 1) * BLK, :], rhs)
            for ref, (_, first) in zip(got, adds):
                if first <= m * BLK < first + ref.shape[0]:
                    value = value + ref[m * BLK - first : (m + 1) * BLK - first, :].astype(F32)
            result[m * BLK : (m + 1) * BLK, :] = value.astype(dtype)

    flops = 2 * RB * FEAT * (hi - lo)
    return call(kernel, out(hi - lo, dtype), 0, flops, dense_t[dz], *grads, *[v for v, _ in adds])


def shards(features, weight, cotangent, blocks, block_scales, block_rows, block_cols, block_counts):
    cnt = block_counts.reshape(1)
    pos = jnp.stack([lax.axis_index(a) for a in ("z", "y", "x", "c")]).astype(jnp.int32)
    tables = (block_rows.reshape(-1), block_cols.reshape(-1), pos, block_scales.reshape(-1))
    blk = blocks[0, 0]
    ys = [hop(features, "y", -d) for d in range(1, NY)]
    a0 = features
    au1, ad1 = hop(a0, "z", 1), hop(a0, "z", -1)
    b0 = jnp.concatenate(ys, axis=0)
    bu1, bd1 = hop(b0, "z", 1), hop(b0, "z", -1)
    dense = build_dense(cnt, *tables, blk)
    au2, ad2 = hop(au1, "z", 1), hop(ad1, "z", -1)
    bu2, bd2 = hop(bu1, "z", 1), hop(bd1, "z", -1)
    acc = forward(dense, [(0, 0, BLK), (0, BLK, YB)], [a0, b0], None, False)
    au3, ad3 = hop(au2, "z", 1), hop(ad2, "z", -1)
    spans = lambda u, d: [(u, 0, BLK), (d, 0, BLK), (u, BLK, YB), (d, BLK, YB)]
    acc = forward(dense, spans(7, 1), [au1, ad1, bu1, bd1], acc, False)
    dense_t = build_dense_t(after(cnt, acc[0, 0]), *tables, blk)
    bu3, bd3 = hop(bu2, "z", 1), hop(bd2, "z", -1)
    a4 = hop(au3, "z", 1)
    acc = forward(dense, spans(6, 2), [au2, ad2, bu2, bd2], acc, False)
    bu4, bd4 = hop(bu3[:BLK], "z", 1), hop(bd3[BLK:], "z", -1)
    acc = forward(dense, spans(5, 3), [au3, ad3, bu3, bd3], acc, False)
    last = [(4, 0, BLK), (4, BLK, 2 * BLK), (4, 2 * BLK, YB)]
    acc, dense_t = lax.optimization_barrier((acc, dense_t))
    mine, theirs = forward(dense, last, [a4, bu4, bd4], acc, True)
    mine = mine + hop(theirs, "c", 1).astype(F32)
    sent = mine.astype(BF)
    parts = [hop(sent[d * BLK : (d + 1) * BLK], "x", d) for d in range(1, NX)]
    hid = mine[:BLK]
    for p in parts:
        hid = hid + p.astype(F32)
    hid = hid.astype(BF)
    agg = mm(hid, weight)
    sig = jax.nn.sigmoid(agg)
    activated = (agg * sig).astype(BF)
    pre = (cotangent.astype(F32) * (sig * (1.0 + agg * (1.0 - sig)))).astype(BF)
    grad = lax.dot_general(pre, weight, (((1,), (1,)), ((), ())), preferred_element_type=F32).astype(BF)
    grads = [grad] + [hop(grad, "x", -d) for d in range(1, NX)]
    grads = grads + [hop(g, "c", 1) for g in grads]

    def step(dz, lo, hi, *adds, dtype=BF):
        return backward(dense_t, grads, dz, lo * BLK, hi * BLK, adds, dtype)

    bu = hop(step(4, 1, 2), "z", 1)
    bd = hop(step(4, 2, 4), "z", -1)
    au = hop(step(4, 0, 1), "z", 1)
    ad = None
    count = NZ * NY * NX * NC
    k = jnp.arange(FEAT, dtype=jnp.int32)
    dest, low = k // 2, k % 2
    order = ((dest % (NX * NC)) * (NZ * NY) + dest // (NX * NC)) * 2 + low
    shuffle = (order[:, None] == k[None, :]).astype(BF)
    wgrad = lax.dot_general(
        mm(hid, shuffle).astype(BF), pre, (((0,), (0,)), ((), ())), preferred_element_type=F32
    ).astype(BF)
    for d in (3, 2, 1):
        bu_sent = step(d, 1, 4, (bu, 0))
        bd_sent = step(NZ - d, 1, 4, (bd, BLK if d == 3 else 0))
        bu, bd = hop(bu_sent, "z", 1), hop(bd_sent, "z", -1)
        au_sent = step(d, 0, 1, (au, 0))
        ad_sent = step(NZ - d, 0, 1, *(() if ad is None else ((ad, 0),)))
        au, ad = hop(au_sent, "z", 1), hop(ad_sent, "z", -1)
        if d == 3:
            wgrad = after(wgrad, bu_sent, bd_sent, au_sent, ad_sent)
            wgrad = lax.all_to_all(wgrad.reshape(NX * NC, 2 * NZ * NY, FEAT), COL, 0, 0)
        if d == 2:
            total = wgrad[0].astype(F32)
            for i in range(1, NX * NC):
                total = total + wgrad[i].astype(F32)
            wgrad = after(total.astype(BF), bu_sent, bd_sent, au_sent, ad_sent)
            wgrad = lax.all_to_all(wgrad.reshape(NZ * NY, 2, FEAT), ROW, 0, 0)
    total = step(0, 1, 4, (bu, 0), (bd, 0))
    parts = [hop(total[(d - 1) * BLK : d * BLK], "y", d) for d in range(1, NY)]
    input_grad = step(0, 0, 1, (au, 0), (ad, 0), dtype=F32)
    for p in parts:
        input_grad = input_grad + p.astype(F32)
    weight_grad = jnp.sum(wgrad.astype(F32), axis=0) * (1.0 / math.sqrt(BLK * count))
    return (activated, input_grad.astype(BF), weight_grad)


def solution(mesh):
    mesh4 = Mesh(np.asarray(mesh.devices).reshape(NZ, NY, NX, NC), ("z", "y", "x", "c"))
    return jax.shard_map(
        shards,
        mesh=mesh4,
        in_specs=(
            P(COL + ROW, None),
            P(),
            P(ROW + COL, None),
            P(ROW, COL, None, None, None),
            P(ROW, COL, None),
            P(ROW, COL, None),
            P(ROW, COL, None),
            P(ROW, COL),
        ),
        out_specs=(P(ROW + COL, None), P(COL + ROW, None), P(ROW + COL, None)),
        check_vma=False,
    )
```
